16 devices in a mesh: z: 2 (over z), y: 2 (over y), xc: 4 (over x, core).
Axes of the slice: x: 2, y: 2, z: 2, core: 2. Of those that a mesh axis runs over, the one named last changes fastest.
Arguments:
- tokens_x: bfloat16 [131072, 768], P(('z', 'y', 'xc'))
- grad_y: bfloat16 [131072, 768], P(('z', 'y', 'xc'))
- w_one: bfloat16 [768, 3072], replicated
- w_two: bfloat16 [3072, 768], replicated
- w_three: bfloat16 [768, 3072], replicated
- w_four: bfloat16 [3072, 768], replicated
Outputs:
- output 1: float32 [768, 3072], replicated
- output 2: float32 [3072, 768], replicated
- output 3: float32 [768, 3072], replicated
- output 4: float32 [3072, 768], replicated
All inputs are finite; a program needn't handle non-finite values.
Results may differ from the reference program's by a relative error of at most 0.00304.
Values are sent between devices in bfloat16 or wider.
A program may use at most 1 GiB of HBM per device.

```python
import math
import jax
import jax.numpy as jnp
from jax import lax

D = 768
FF = 3072
TOKENS_DEV = 8192
DEVICES = 16

TOKENS = DEVICES * TOKENS_DEV
GELU_SCALE = math.sqrt(2.0 / math.pi)
GELU_CUBIC = 0.044715


def gelu_value(pre_act):
    return 0.5 * pre_act * (1.0 + jnp.tanh(GELU_SCALE * (pre_act + GELU_CUBIC * pre_act * pre_act * pre_act)))


def gelu_grad(pre_act):
    tanh_val = jnp.tanh(GELU_SCALE * (pre_act + GELU_CUBIC * pre_act * pre_act * pre_act))
    return 0.5 * (1.0 + tanh_val) + 0.5 * pre_act * (1.0 - tanh_val * tanh_val) * GELU_SCALE * (1.0 + 3.0 * GELU_CUBIC * pre_act * pre_act)


def setup_inputs(seed: int = 0) -> dict:
    root_key = jax.random.key(seed)
    key_list = jax.random.split(root_key, 8)
    scale_x = jax.random.uniform(key_list[0], (DEVICES, 1, 1), jnp.float32, 0.7, 1.3)
    scale_g = jax.random.uniform(key_list[1], (DEVICES, 1, 1), jnp.float32, 0.7, 1.3)
    x_rows = jax.random.normal(key_list[2], (DEVICES, TOKENS_DEV, D), jnp.float32) * scale_x
    g_rows = jax.random.normal(key_list[3], (DEVICES, TOKENS_DEV, D), jnp.float32) * scale_g
    w_one = jax.random.normal(key_list[4], (D, FF), jnp.float32) * D ** -0.5
    w_two = jax.random.normal(key_list[5], (FF, D), jnp.float32) * FF ** -0.5
    w_three = jax.random.normal(key_list[6], (D, FF), jnp.float32) * D ** -0.5
    w_four = jax.random.normal(key_list[7], (FF, D), jnp.float32) * FF ** -0.5
    return {
        "tokens_x": x_rows.reshape(TOKENS, D).astype(jnp.bfloat16),
        "grad_y": g_rows.reshape(TOKENS, D).astype(jnp.bfloat16),
        "w_one": w_one.astype(jnp.bfloat16),
        "w_two": w_two.astype(jnp.bfloat16),
        "w_three": w_three.astype(jnp.bfloat16),
        "w_four": w_four.astype(jnp.bfloat16),
    }


def local_grads(x_loc, g_loc, w_one, w_two, w_three, w_four):
    a_one = jnp.dot(x_loc, w_one, preferred_element_type=jnp.float32).astype(jnp.bfloat16)
    h_one = gelu_value(a_one.astype(jnp.float32)).astype(jnp.bfloat16)
    h_two = (jnp.dot(h_one, w_two, preferred_element_type=jnp.float32) + x_loc.astype(jnp.float32)).astype(jnp.bfloat16)
    a_three = jnp.dot(h_two, w_three, preferred_element_type=jnp.float32).astype(jnp.bfloat16)
    h_three = gelu_value(a_three.astype(jnp.float32)).astype(jnp.bfloat16)
    d_w4 = jnp.dot(h_three.T, g_loc, preferred_element_type=jnp.float32)
    d_a3 = (jnp.dot(g_loc, w_four.T, preferred_element_type=jnp.float32) * gelu_grad(a_three.astype(jnp.float32))).astype(jnp.bfloat16)
    d_w3 = jnp.dot(h_two.T, d_a3, preferred_element_type=jnp.float32)
    d_h2 = (jnp.dot(d_a3, w_three.T, preferred_element_type=jnp.float32) + g_loc.astype(jnp.float32)).astype(jnp.bfloat16)
    d_w2 = jnp.dot(h_one.T, d_h2, preferred_element_type=jnp.float32)
    d_a1 = (jnp.dot(d_h2, w_two.T, preferred_element_type=jnp.float32) * gelu_grad(a_one.astype(jnp.float32))).astype(jnp.bfloat16)
    d_w1 = jnp.dot(x_loc.T, d_a1, preferred_element_type=jnp.float32)
    return d_w1, d_w2, d_w3, d_w4


def reference(tokens_x, grad_y, w_one, w_two, w_three, w_four):
    x_shards = tokens_x.reshape(DEVICES, TOKENS_DEV, D)
    g_shards = grad_y.reshape(DEVICES, TOKENS_DEV, D)

    def accumulate(running, pair):
        x_loc, g_loc = pair
        grads = local_grads(x_loc, g_loc, w_one, w_two, w_three, w_four)
        return tuple(acc + new for acc, new in zip(running, grads)), None

    start_sums = (
        jnp.zeros((D, FF), jnp.float32),
        jnp.zeros((FF, D), jnp.float32),
        jnp.zeros((D, FF), jnp.float32),
        jnp.zeros((FF, D), jnp.float32),
    )
    totals, _ = lax.scan(accumulate, start_sums, (x_shards, g_shards))
    return (totals[0] / DEVICES, totals[1] / DEVICES, totals[2] / DEVICES, totals[3] / DEVICES)
```

```python
import functools
import math
import jax
import jax.numpy as jnp
from jax import lax
from jax.experimental import pallas as pl
from jax.experimental.pallas import tpu as pltpu
from jax.sharding import PartitionSpec as P

GELU_SCALE = math.sqrt(2.0 / math.pi)
GELU_CUBIC = 0.044715
F32 = jnp.float32
BF16 = jnp.bfloat16
MESH = pl.DeviceIdType.MESH
COLORS = 3
CHUNKS = 4
TILE = 512
RS_STEPS = (0, 2, 7, 11, 13)
AG_STEPS = (0, 2, 6, 11, 13, 15)
MID_RS_STEPS = (0, 2, 6, 8, 9)
MID_AG_STEPS = (0, 2, 4, 7, 9, 15)
MID_LAST_STEPS = (9, 11, 12, 15)


def dot(a, b):
    return jnp.dot(a, b, preferred_element_type=F32)


def dot_rows(a, b):
    return lax.dot_general(a, b, (((0,), (0,)), ((), ())), preferred_element_type=F32)


def gelu_tanh(pre_act, square):
    return jnp.tanh(pre_act * (GELU_SCALE + (GELU_SCALE * GELU_CUBIC) * square))


def gelu_value(pre_act):
    return (0.5 * pre_act) * (1.0 + gelu_tanh(pre_act, pre_act * pre_act))


def gelu_both(pre_act):
    square = pre_act * pre_act
    tanh_val = gelu_tanh(pre_act, square)
    half = 0.5 * pre_act
    value = half * (1.0 + tanh_val)
    slope = (0.5 + 0.5 * tanh_val) + (half * (1.0 - tanh_val * tanh_val)) * (GELU_SCALE + (3.0 * GELU_SCALE * GELU_CUBIC) * square)
    return value, slope


class Reducer:
    def __init__(self, n_dev, q, full, b0, b1, b2, b3, rs_send, rs_recv, ag_send, ag_recv, out_sem, carry_sem):
        self.q, self.full, self.bufs, self.n_dev = q, full, (b0, b1, b2, b3), n_dev
        self.out_sem, self.carry_sem = out_sem, carry_sem
        self.rs_send, self.rs_recv, self.ag_send, self.ag_recv = rs_send, rs_recv, ag_send, ag_recv
        self.side = q.shape[2]
        z, y, xc = lax.axis_index("z"), lax.axis_index("y"), lax.axis_index("xc")
        x, core = xc // 2, xc % 2
        self.core = core
        self.bits = (x, y, z)
        self.peers = (
            (z, y, (1 - x) * 2 + core),
            (z, 1 - y, xc),
            (1 - z, y, xc),
        )
        self.other_core = (z, y, x * 2 + (1 - core))

    def barrier(self):
        sem = pltpu.get_barrier_semaphore()
        for peer in self.peers + (self.other_core,):
            pl.semaphore_signal(sem, inc=1, device_id=peer, device_id_type=MESH)
        pl.semaphore_wait(sem, 4)

    def rows(self, color, depth):
        count = self.side // COLORS
        start = self.core * self.side + color * count
        for level in range(depth):
            count //= 2
            start = start + self.bits[(color + level) % 3] * count
        return start, count

    def part(self, ref, par, start, count):
        return ref.at[par, pl.ds(pl.multiple_of(start, 32), count), :]

    def rs_copy(self, stage, color, chunk):
        par = chunk % 2
        if stage == 0:
            count = self.side // COLORS
            start = (1 - self.core) * self.side + color * count
            peer = self.other_core
        else:
            axis = (color + stage - 1) % 3
            start, count = self.rows(color, stage - 1)
            count //= 2
            start = start + (1 - self.bits[axis]) * count
            peer = self.peers[axis]
        return pltpu.make_async_remote_copy(
            src_ref=self.part(self.q, par, start, count),
            dst_ref=self.bufs[stage].at[par, color],
            send_sem=self.rs_send.at[stage, color],
            recv_sem=self.rs_recv.at[par, stage, color],
            device_id=peer,
            device_id_type=MESH,
        )

    def rs(self, stage, chunk):
        par = chunk % 2
        for color in range(COLORS):
            if stage > 0:
                self.rs_copy(stage - 1, color, chunk).wait()
                start, count = self.rows(color, stage - 1)
                part = self.part(self.q, par, start, count)
                total = part[...] + self.bufs[stage - 1][par, color]
                if stage == 4:
                    self.part(self.full, par, start, count)[...] = total * (1.0 / self.n_dev)
                else:
                    part[...] = total
            if stage < 4:
                self.rs_copy(stage, color, chunk).start()

    def ag_copy(self, stage, color, chunk):
        par = chunk % 2
        start, count = self.rows(color, 3 - stage)
        peer = self.other_core if stage == 3 else self.peers[(color + 2 - stage) % 3]
        part = self.part(self.full, par, start, count)
        return pltpu.make_async_remote_copy(
            src_ref=part,
            dst_ref=part,
            send_sem=self.ag_send.at[stage, color],
            recv_sem=self.ag_recv.at[par, stage, color],
            device_id=peer,
            device_id_type=MESH,
        )

    def ag(self, stage, chunk):
        for color in range(COLORS):
            if stage > 0:
                self.ag_copy(stage - 1, color, chunk).wait()
            if stage < 4:
                self.ag_copy(stage, color, chunk).start()


    def out_copies(self, chunk, index, rows_out, cols_out):
        par, side = chunk % 2, self.side
        span = pl.ds(pl.multiple_of(index * side, side), side)
        return (
            pltpu.make_async_copy(self.full.at[par, pl.ds(0, side), :], rows_out.at[span, :], self.out_sem.at[par, 0]),
            pltpu.make_async_copy(self.full.at[par, pl.ds(side, side), :], cols_out.at[:, span], self.out_sem.at[par, 1]),
        )

    def carry_copies(self, chunk, partial, pieces, load):
        pairs = [(self.q.at[chunk % 2], partial)]
        for color in range(COLORS):
            start, count = self.rows(color, 3)
            pairs.append((self.part(self.full, (chunk - 1) % 2, start, count), pieces.at[color]))
        return [
            pltpu.make_async_copy(far if load else near, near if load else far, self.carry_sem.at[k])
            for k, (near, far) in enumerate(pairs)
        ]


def run(copies):
    for copy in copies:
        copy.start()
    for copy in copies:
        copy.wait()


def chunk_events(red, j, r, rows_out, cols_out):
    @pl.when(jnp.logical_and(j == 0, r == 0))
    def _():
        red.barrier()

    for stage, step in enumerate(RS_STEPS):
        @pl.when(jnp.logical_and(j >= 1, r == step))
        def _():
            red.rs(stage, j - 1)

    for stage, step in enumerate(AG_STEPS):
        @pl.when(jnp.logical_and(j >= 2, r == step))
        def _():
            if stage < 5:
                red.ag(stage, j - 2)
            if stage >= 4:
                for copy in red.out_copies(j - 2, j - 2, rows_out, cols_out):
                    copy.start() if stage == 4 else copy.wait()


def forward_kernel(x_ref, w1_ref, w2_ref, a1_ref, h2_ref):
    width = w1_ref.shape[1] // CHUNKS
    x = x_ref[...]
    total = x.astype(F32)
    for c in range(CHUNKS):
        cols = slice(c * width, (c + 1) * width)
        a = dot(x, w1_ref[:, cols]).astype(BF16)
        a1_ref[:, cols] = a
        total = total + dot(gelu_value(a.astype(F32)).astype(BF16), w2_ref[cols, :])
    h2_ref[...] = total.astype(BF16)


def upper_kernel(n_dev, steps, h2_ref, g_ref, w3_ref, w4t_ref, da3_ref, rows_out, cols_out, partial_out, pieces_out, *refs):
    j, r = pl.program_id(0), pl.program_id(1)
    red = Reducer(n_dev, *refs)
    q, side, slot = red.q, red.side, j % 2
    chunk_events(red, j, r, rows_out, cols_out)

    @pl.when(r == 0)
    def _():
        q[slot] = jnp.zeros(q.shape[1:], F32)

    h2, g = h2_ref[...], g_ref[...]
    a3 = dot(h2, w3_ref[...]).astype(BF16)
    back = dot(g, w4t_ref[...])
    value, slope = gelu_both(a3.astype(F32))
    h3 = value.astype(BF16)
    da3 = (back * slope).astype(BF16)
    da3_ref[...] = da3
    q[slot, 0:side, :] += dot_rows(h3, g)
    q[slot, side:2 * side, :] += dot_rows(h2, da3)

    @pl.when(jnp.logical_and(j == CHUNKS - 1, r == steps - 1))
    def _():
        run(red.carry_copies(CHUNKS - 1, partial_out, pieces_out, False))


def middle_kernel(n_dev, steps, da3_ref, w3_ref, g_ref, partial_ref, pieces_ref, dh2_ref, rows_out, cols_out, *refs):
    r = pl.program_id(0)
    red = Reducer(n_dev, *refs)
    last = CHUNKS - 1

    @pl.when(r == 0)
    def _():
        run(red.carry_copies(last, partial_ref, pieces_ref, True))
        red.barrier()

    for stage, step in enumerate(MID_RS_STEPS):
        @pl.when(r == step)
        def _():
            red.rs(stage, last)

    for stage, step in enumerate(MID_AG_STEPS):
        @pl.when(r == step)
        def _():
            if stage < 5:
                red.ag(stage, last - 1)
            if stage >= 4:
                for copy in red.out_copies(last - 1, 0, rows_out, cols_out):
                    copy.start() if stage == 4 else copy.wait()

    for stage, step in enumerate(MID_LAST_STEPS):
        @pl.when(r == step)
        def _():
            red.ag(stage, last)

    back = lax.dot_general(da3_ref[...], w3_ref[...], (((1,), (1,)), ((), ())), preferred_element_type=F32)
    dh2_ref[...] = (back + g_ref[...].astype(F32)).astype(BF16)

    @pl.when(r == steps - 1)
    def _():
        red.ag(4, last)
        run(red.out_copies(last, 1, rows_out, cols_out))


def lower_kernel(n_dev, steps, x_ref, dh2_ref, a1_ref, w2t_ref, rows_out, cols_out, *refs):
    j, r = pl.program_id(0), pl.program_id(1)
    red = Reducer(n_dev, *refs)
    q, side, slot = red.q, red.side, j % 2
    chunk_events(red, j, r, rows_out, cols_out)

    @pl.when(r == 0)
    def _():
        q[slot] = jnp.zeros(q.shape[1:], F32)

    x, dh2 = x_ref[...], dh2_ref[...]
    back = dot(dh2, w2t_ref[...])
    value, slope = gelu_both(a1_ref[...].astype(F32))
    h1 = value.astype(BF16)
    da1 = (back * slope).astype(BF16)
    q[slot, 0:side, :] += dot_rows(h1, dh2)
    q[slot, side:2 * side, :] += dot_rows(x, da1)

    @pl.when(jnp.logical_and(j == CHUNKS - 1, r == steps - 1))
    def _():
        last = CHUNKS - 1
        for stage in range(5):
            red.rs(stage, last)
            red.ag(stage, last - 1)
        first = red.out_copies(last - 1, last - 1, rows_out, cols_out)
        for copy in first:
            copy.start()
        for stage in range(5):
            red.ag(stage, last)
        run(red.out_copies(last, last, rows_out, cols_out))
        for copy in first:
            copy.wait()


def scratch(side):
    part = side // COLORS
    return [
        pltpu.VMEM((2, 2 * side, side), F32),
        pltpu.VMEM((2, 2 * side, side), F32),
        pltpu.VMEM((2, COLORS, part, side), F32),
        pltpu.VMEM((2, COLORS, part // 2, side), F32),
        pltpu.VMEM((2, COLORS, part // 4, side), F32),
        pltpu.VMEM((2, COLORS, part // 8, side), F32),
        pltpu.SemaphoreType.DMA((4, COLORS)),
        pltpu.SemaphoreType.DMA((2, 4, COLORS)),
        pltpu.SemaphoreType.DMA((4, COLORS)),
        pltpu.SemaphoreType.DMA((2, 4, COLORS)),
        pltpu.SemaphoreType.DMA((2, 2)),
        pltpu.SemaphoreType.DMA((4,)),
    ]


def solution(mesh):
    n_dev = math.prod(mesh.shape.values())
    batch_spec = P(("z", "y", "xc"), None)
    whole_spec = P(None, None)

    def device_step(x, g, w_one, w_two, w_three, w_four):
        n, d = x.shape
        ff = w_one.shape[1]
        steps = n // TILE
        side = ff // CHUNKS
        any_spec = pl.BlockSpec(memory_space=pl.ANY)

        def params(collective=None):
            if collective is None:
                return pltpu.CompilerParams(vmem_limit_bytes=60 * 2**20)
            return pltpu.CompilerParams(vmem_limit_bytes=62 * 2**20, collective_id=collective, has_side_effects=True)

        a_one, h_two = pl.pallas_call(
            forward_kernel,
            grid=(steps,),
            in_specs=[
                pl.BlockSpec((TILE, d), lambda r: (r, 0)),
                pl.BlockSpec((d, ff), lambda r: (0, 0)),
                pl.BlockSpec((ff, d), lambda r: (0, 0)),
            ],
            out_specs=[pl.BlockSpec((TILE, ff), lambda r: (r, 0)), pl.BlockSpec((TILE, d), lambda r: (r, 0))],
            out_shape=[jax.ShapeDtypeStruct((n, ff), BF16), jax.ShapeDtypeStruct((n, d), BF16)],
            compiler_params=params(),
            name="forward",
        )(x, w_one, w_two)

        tile_spec = pl.BlockSpec((TILE, d), lambda j, r: (r, 0))
        col_spec = pl.BlockSpec((TILE, side), lambda j, r: (r, j))
        w_spec = pl.BlockSpec((d, side), lambda j, r: (0, j))

        half_rows = jax.ShapeDtypeStruct((2 * side, d), F32)
        half_cols = jax.ShapeDtypeStruct((d, 2 * side), F32)

        d_a3, w4_a, w3_a, partial, pieces = pl.pallas_call(
            functools.partial(upper_kernel, n_dev, steps),
            grid=(CHUNKS, steps),
            in_specs=[tile_spec, tile_spec, w_spec, w_spec],
            out_specs=[col_spec] + [any_spec] * 4,
            out_shape=[
                jax.ShapeDtypeStruct((n, ff), BF16),
                half_rows,
                half_cols,
                jax.ShapeDtypeStruct((2 * side, side), F32),
                jax.ShapeDtypeStruct((COLORS, side // COLORS // 8, side), F32),
            ],
            scratch_shapes=scratch(side),
            compiler_params=params(0),
            name="upper",
        )(h_two, g, w_three, w_four.T)

        d_h2, w4_b, w3_b = pl.pallas_call(
            functools.partial(middle_kernel, n_dev, steps),
            grid=(steps,),
            in_specs=[
                pl.BlockSpec((TILE, ff), lambda r: (r, 0)),
                pl.BlockSpec((d, ff), lambda r: (0, 0)),
                pl.BlockSpec((TILE, d), lambda r: (r, 0)),
                any_spec,
                any_spec,
            ],
            out_specs=[pl.BlockSpec((TILE, d), lambda r: (r, 0)), any_spec, any_spec],
            out_shape=[jax.ShapeDtypeStruct((n, d), BF16), half_rows, half_cols],
            scratch_shapes=scratch(side),
            compiler_params=params(1),
            name="middle",
        )(d_a3, w_three, g, partial, pieces)

        grad_w2, grad_w1 = pl.pallas_call(
            functools.partial(lower_kernel, n_dev, steps),
            grid=(CHUNKS, steps),
            in_specs=[tile_spec, tile_spec, col_spec, w_spec],
            out_specs=[any_spec] * 2,
            out_shape=[jax.ShapeDtypeStruct((ff, d), F32), jax.ShapeDtypeStruct((d, ff), F32)],
            scratch_shapes=scratch(side),
            compiler_params=params(2),
            name="lower",
        )(x, d_h2, a_one, w_two.T)

        grad_w4 = jnp.concatenate([w4_a, w4_b], axis=0)
        grad_w3 = jnp.concatenate([w3_a, w3_b], axis=1)
        return grad_w1, grad_w2, grad_w3, grad_w4

    return jax.shard_map(
        device_step,
        mesh=mesh,
        in_specs=(batch_spec, batch_spec, whole_spec, whole_spec, whole_spec, whole_spec),
        out_specs=(whole_spec, whole_spec, whole_spec, whole_spec),
        check_vma=False,
    )
```

```python
import functools
import math
import jax
import jax.numpy as jnp
from jax import lax
from jax.experimental import pallas as pl
from jax.experimental.pallas import tpu as pltpu
from jax.sharding import PartitionSpec as P

GELU_SCALE = math.sqrt(2.0 / math.pi)
GELU_CUBIC = 0.044715
F32 = jnp.float32
BF16 = jnp.bfloat16
MESH = pl.DeviceIdType.MESH
COLORS = 3
CHUNKS = 4
TILE = 512
UP_TILE = 1024
LOW_TILE = 1024
TRANS_B = True
RS_STEPS = (0, 1, 4, 7, 0)
AG_STEPS = (0, 1, 4, 7, 1, 3)
MID_RS_STEPS = (0, 2, 6, 9, 10)
MID_AG_STEPS = (0, 2, 6, 10, 12, 15)
MID_LAST_STEPS = (10, 12, 14, 15)


def dot(a, b):
    return jnp.dot(a, b, preferred_element_type=F32)


def dot_rows(a, b):
    return lax.dot_general(a, b, (((0,), (0,)), ((), ())), preferred_element_type=F32)


def dot_back(a, w):
    return lax.dot_general(a, w, (((1,), (1 if TRANS_B else 0,)), ((), ())), preferred_element_type=F32)


def gelu_tanh(pre_act, square):
    return jnp.tanh(pre_act * (GELU_SCALE + (GELU_SCALE * GELU_CUBIC) * square))


def gelu_value(pre_act):
    return (0.5 * pre_act) * (1.0 + gelu_tanh(pre_act, pre_act * pre_act))


def gelu_both(pre_act):
    square = pre_act * pre_act
    tanh_val = gelu_tanh(pre_act, square)
    half = 0.5 * pre_act
    value = half * (1.0 + tanh_val)
    slope = (0.5 + 0.5 * tanh_val) + (half * (1.0 - tanh_val * tanh_val)) * (GELU_SCALE + (3.0 * GELU_SCALE * GELU_CUBIC) * square)
    return value, slope


class Reducer:
    def __init__(self, n_dev, q, full, b0, b1, b2, b3, rs_send, rs_recv, ag_send, ag_recv, out_sem, carry_sem):
        self.q, self.full, self.bufs, self.n_dev = q, full, (b0, b1, b2, b3), n_dev
        self.out_sem, self.carry_sem = out_sem, carry_sem
        self.rs_send, self.rs_recv, self.ag_send, self.ag_recv = rs_send, rs_recv, ag_send, ag_recv
        self.side = q.shape[2]
        z, y, xc = lax.axis_index("z"), lax.axis_index("y"), lax.axis_index("xc")
        x, core = xc // 2, xc % 2
        self.core = core
        self.bits = (x, y, z)
        self.peers = (
            (z, y, (1 - x) * 2 + core),
            (z, 1 - y, xc),
            (1 - z, y, xc),
        )
        self.other_core = (z, y, x * 2 + (1 - core))

    def barrier(self):
        sem = pltpu.get_barrier_semaphore()
        for peer in self.peers + (self.other_core,):
            pl.semaphore_signal(sem, inc=1, device_id=peer, device_id_type=MESH)
        pl.semaphore_wait(sem, 4)

    def rows(self, color, depth):
        count = self.side // COLORS
        start = self.core * self.side + color * count
        for level in range(depth):
            count //= 2
            start = start + self.bits[(color + level) % 3] * count
        return start, count

    def part(self, ref, par, start, count):
        return ref.at[par, pl.ds(pl.multiple_of(start, 32), count), :]

    def rs_copy(self, stage, color, chunk):
        par = chunk % 2
        if stage == 0:
            count = self.side // COLORS
            start = (1 - self.core) * self.side + color * count
            peer = self.other_core
        else:
            axis = (color + stage - 1) % 3
            start, count = self.rows(color, stage - 1)
            count //= 2
            start = start + (1 - self.bits[axis]) * count
            peer = self.peers[axis]
        return pltpu.make_async_remote_copy(
            src_ref=self.part(self.q, par, start, count),
            dst_ref=self.bufs[stage].at[par, color],
            send_sem=self.rs_send.at[stage, color],
            recv_sem=self.rs_recv.at[par, stage, color],
            device_id=peer,
            device_id_type=MESH,
        )

    def rs(self, stage, chunk):
        par = chunk % 2
        for color in range(COLORS):
            if stage > 0:
                self.rs_copy(stage - 1, color, chunk).wait()
                start, count = self.rows(color, stage - 1)
                part = self.part(self.q, par, start, count)
                total = part[...] + self.bufs[stage - 1][par, color]
                if stage == 4:
                    self.part(self.full, par, start, count)[...] = total * (1.0 / self.n_dev)
                else:
                    part[...] = total
            if stage < 4:
                self.rs_copy(stage, color, chunk).start()

    def ag_copy(self, stage, color, chunk):
        par = chunk % 2
        start, count = self.rows(color, 3 - stage)
        peer = self.other_core if stage == 3 else self.peers[(color + 2 - stage) % 3]
        part = self.part(self.full, par, start, count)
        return pltpu.make_async_remote_copy(
            src_ref=part,
            dst_ref=part,
            send_sem=self.ag_send.at[stage, color],
            recv_sem=self.ag_recv.at[par, stage, color],
            device_id=peer,
            device_id_type=MESH,
        )

    def ag(self, stage, chunk):
        for color in range(COLORS):
            if stage > 0:
                self.ag_copy(stage - 1, color, chunk).wait()
            if stage < 4:
                self.ag_copy(stage, color, chunk).start()


    def out_copies(self, chunk, index, rows_out, cols_out):
        par, side = chunk % 2, self.side
        span = pl.ds(pl.multiple_of(index * side, side), side)
        return (
            pltpu.make_async_copy(self.full.at[par, pl.ds(0, side), :], rows_out.at[span, :], self.out_sem.at[par, 0]),
            pltpu.make_async_copy(self.full.at[par, pl.ds(side, side), :], cols_out.at[:, span], self.out_sem.at[par, 1]),
        )

    def carry_copies(self, chunk, partial, pieces, load):
        pairs = [(self.q.at[chunk % 2], partial)]
        for color in range(COLORS):
            start, count = self.rows(color, 3)
            pairs.append((self.part(self.full, (chunk - 1) % 2, start, count), pieces.at[color]))
        return [
            pltpu.make_async_copy(far if load else near, near if load else far, self.carry_sem.at[k])
            for k, (near, far) in enumerate(pairs)
        ]


def run(copies):
    for copy in copies:
        copy.start()
    for copy in copies:
        copy.wait()


def chunk_events(red, j, r, rows_out, cols_out):
    @pl.when(jnp.logical_and(j == 0, r == 0))
    def _():
        red.barrier()

    @pl.when(jnp.logical_and(j >= 2, r == RS_STEPS[4]))
    def _():
        red.rs(4, j - 2)

    for stage in range(4):
        @pl.when(jnp.logical_and(j >= 1, r == RS_STEPS[stage]))
        def _():
            red.rs(stage, j - 1)

        @pl.when(jnp.logical_and(j >= 2, r == AG_STEPS[stage]))
        def _():
            red.ag(stage, j - 2)

    @pl.when(jnp.logical_and(j >= 3, r == AG_STEPS[4]))
    def _():
        red.ag(4, j - 3)
        for copy in red.out_copies(j - 3, j - 3, rows_out, cols_out):
            copy.start()

    @pl.when(jnp.logical_and(j >= 3, r == AG_STEPS[5]))
    def _():
        for copy in red.out_copies(j - 3, j - 3, rows_out, cols_out):
            copy.wait()


def forward_kernel(x_ref, w1_ref, w2_ref, a1_ref, h2_ref):
    width = w1_ref.shape[1] // CHUNKS
    x = x_ref[...]
    total = x.astype(F32)
    for c in range(CHUNKS):
        cols = slice(c * width, (c + 1) * width)
        a = dot(x, w1_ref[:, cols]).astype(BF16)
        a1_ref[:, cols] = a
        total = total + dot(gelu_value(a.astype(F32)).astype(BF16), w2_ref[cols, :])
    h2_ref[...] = total.astype(BF16)


def upper_kernel(n_dev, steps, h2_ref, g_ref, w3_ref, w4t_ref, da3_ref, rows_out, cols_out, partial_out, pieces_out, h3_buf, *refs):
    j, r = pl.program_id(0), pl.program_id(1)
    red = Reducer(n_dev, *refs)
    q, side, slot = red.q, red.side, j % 2
    chunk_events(red, j, r, rows_out, cols_out)

    @pl.when(r == 0)
    def _():
        q[slot] = jnp.zeros(q.shape[1:], F32)

    for start in range(0, h2_ref.shape[0], TILE):
        span = slice(start, start + TILE)
        a3 = dot(h2_ref[span, :], w3_ref[...]).astype(BF16)
        back = dot_back(g_ref[span, :], w4t_ref[...])
        value, slope = gelu_both(a3.astype(F32))
        h3_buf[span, :] = value.astype(BF16)
        da3_ref[span, :] = (back * slope).astype(BF16)
    q[slot, 0:side, :] += dot_rows(h3_buf[...], g_ref[...])
    q[slot, side:2 * side, :] += dot_rows(h2_ref[...], da3_ref[...])

    @pl.when(jnp.logical_and(j == CHUNKS - 1, r == steps - 1))
    def _():
        last = CHUNKS - 1
        red.rs(4, last - 1)
        red.ag(4, last - 2)
        run(list(red.out_copies(last - 2, last - 2, rows_out, cols_out)) + red.carry_copies(last, partial_out, pieces_out, False))


def middle_kernel(n_dev, steps, da3_ref, w3_ref, g_ref, partial_ref, pieces_ref, dh2_ref, rows_out, cols_out, *refs):
    r = pl.program_id(0)
    red = Reducer(n_dev, *refs)
    last = CHUNKS - 1

    @pl.when(r == 0)
    def _():
        run(red.carry_copies(last, partial_ref, pieces_ref, True))
        red.barrier()

    for stage, step in enumerate(MID_RS_STEPS):
        @pl.when(r == step)
        def _():
            red.rs(stage, last)

    for stage, step in enumerate(MID_AG_STEPS):
        @pl.when(r == step)
        def _():
            if stage < 5:
                red.ag(stage, last - 1)
            if stage >= 4:
                for copy in red.out_copies(last - 1, 0, rows_out, cols_out):
                    copy.start() if stage == 4 else copy.wait()

    for stage, step in enumerate(MID_LAST_STEPS):
        @pl.when(r == step)
        def _():
            red.ag(stage, last)

    back = lax.dot_general(da3_ref[...], w3_ref[...], (((1,), (1,)), ((), ())), preferred_element_type=F32)
    dh2_ref[...] = (back + g_ref[...].astype(F32)).astype(BF16)

    @pl.when(r == steps - 1)
    def _():
        red.ag(4, last)
        run(red.out_copies(last, 1, rows_out, cols_out))


def lower_kernel(n_dev, steps, x_ref, dh2_ref, a1_ref, w2t_ref, rows_out, cols_out, h1_buf, da1_buf, *refs):
    j, r = pl.program_id(0), pl.program_id(1)
    red = Reducer(n_dev, *refs)
    q, side, slot = red.q, red.side, j % 2
    chunk_events(red, j, r, rows_out, cols_out)

    @pl.when(r == 0)
    def _():
        q[slot] = jnp.zeros(q.shape[1:], F32)

    for start in range(0, x_ref.shape[0], TILE):
        span = slice(start, start + TILE)
        back = dot_back(dh2_ref[span, :], w2t_ref[...])
        value, slope = gelu_both(a1_ref[span, :].astype(F32))
        h1_buf[span, :] = value.astype(BF16)
        da1_buf[span, :] = (back * slope).astype(BF16)
    q[slot, 0:side, :] += dot_rows(h1_buf[...], dh2_ref[...])
    q[slot, side:2 * side, :] += dot_rows(x_ref[...], da1_buf[...])

    @pl.when(jnp.logical_and(j == CHUNKS - 1, r == steps - 1))
    def _():
        last = CHUNKS - 1
        outs = [red.out_copies(chunk, chunk, rows_out, cols_out) for chunk in (last - 2, last - 1, last)]
        red.rs(0, last)
        red.rs(4, last - 1)
        red.ag(0, last - 1)
        red.ag(4, last - 2)
        for copy in outs[0]:
            copy.start()
        for stage in range(1, 4):
            red.rs(stage, last)
            red.ag(stage, last - 1)
            if stage == 1:
                for copy in outs[0]:
                    copy.wait()
        red.rs(4, last)
        red.ag(0, last)
        red.ag(4, last - 1)
        for copy in outs[1]:
            copy.start()
        for stage in range(1, 5):
            red.ag(stage, last)
        run(outs[2])
        for copy in outs[1]:
            copy.wait()


def scratch(side):
    part = side // COLORS
    return [
        pltpu.VMEM((2, 2 * side, side), F32),
        pltpu.VMEM((2, 2 * side, side), F32),
        pltpu.VMEM((2, COLORS, part, side), F32),
        pltpu.VMEM((2, COLORS, part // 2, side), F32),
        pltpu.VMEM((2, COLORS, part // 4, side), F32),
        pltpu.VMEM((2, COLORS, part // 8, side), F32),
        pltpu.SemaphoreType.DMA((4, COLORS)),
        pltpu.SemaphoreType.DMA((2, 4, COLORS)),
        pltpu.SemaphoreType.DMA((4, COLORS)),
        pltpu.SemaphoreType.DMA((2, 4, COLORS)),
        pltpu.SemaphoreType.DMA((2, 2)),
        pltpu.SemaphoreType.DMA((4,)),
    ]


def solution(mesh):
    n_dev = math.prod(mesh.shape.values())
    batch_spec = P(("z", "y", "xc"), None)
    whole_spec = P(None, None)

    def device_step(x, g, w_one, w_two, w_three, w_four):
        n, d = x.shape
        ff = w_one.shape[1]
        steps = n // TILE
        side = ff // CHUNKS
        any_spec = pl.BlockSpec(memory_space=pl.ANY)

        def params(collective=None):
            if collective is None:
                return pltpu.CompilerParams(vmem_limit_bytes=60 * 2**20)
            return pltpu.CompilerParams(vmem_limit_bytes=63 * 2**20, collective_id=collective, has_side_effects=True)

        a_one, h_two = pl.pallas_call(
            forward_kernel,
            grid=(steps,),
            in_specs=[
                pl.BlockSpec((TILE, d), lambda r: (r, 0)),
                pl.BlockSpec((d, ff), lambda r: (0, 0)),
                pl.BlockSpec((ff, d), lambda r: (0, 0)),
            ],
            out_specs=[pl.BlockSpec((TILE, ff), lambda r: (r, 0)), pl.BlockSpec((TILE, d), lambda r: (r, 0))],
            out_shape=[jax.ShapeDtypeStruct((n, ff), BF16), jax.ShapeDtypeStruct((n, d), BF16)],
            compiler_params=params(),
            name="forward",
        )(x, w_one, w_two)

        def tile_spec(tile):
            return pl.BlockSpec((tile, d), lambda j, r: (r, 0))

        def col_spec(tile):
            return pl.BlockSpec((tile, side), lambda j, r: (r, j))

        w_spec = pl.BlockSpec((d, side), lambda j, r: (0, j))
        back_spec = pl.BlockSpec((side, d), lambda j, r: (j, 0)) if TRANS_B else w_spec

        half_rows = jax.ShapeDtypeStruct((2 * side, d), F32)
        half_cols = jax.ShapeDtypeStruct((d, 2 * side), F32)

        d_a3, w4_a, w3_a, partial, pieces = pl.pallas_call(
            functools.partial(upper_kernel, n_dev, n // UP_TILE),
            grid=(CHUNKS, n // UP_TILE),
            in_specs=[tile_spec(UP_TILE), tile_spec(UP_TILE), w_spec, back_spec],
            out_specs=[col_spec(UP_TILE)] + [any_spec] * 4,
            out_shape=[
                jax.ShapeDtypeStruct((n, ff), BF16),
                half_rows,
                half_cols,
                jax.ShapeDtypeStruct((2 * side, side), F32),
                jax.ShapeDtypeStruct((COLORS, side // COLORS // 8, side), F32),
            ],
            scratch_shapes=[pltpu.VMEM((UP_TILE, side), BF16)] + scratch(side),
            compiler_params=params(0),
            name="upper",
        )(h_two, g, w_three, w_four if TRANS_B else w_four.T)

        d_h2, w4_b, w3_b = pl.pallas_call(
            functools.partial(middle_kernel, n_dev, steps),
            grid=(steps,),
            in_specs=[
                pl.BlockSpec((TILE, ff), lambda r: (r, 0)),
                pl.BlockSpec((d, ff), lambda r: (0, 0)),
                pl.BlockSpec((TILE, d), lambda r: (r, 0)),
                any_spec,
                any_spec,
            ],
            out_specs=[pl.BlockSpec((TILE, d), lambda r: (r, 0)), any_spec, any_spec],
            out_shape=[jax.ShapeDtypeStruct((n, d), BF16), half_rows, half_cols],
            scratch_shapes=scratch(side),
            compiler_params=params(1),
            name="middle",
        )(d_a3, w_three, g, partial, pieces)

        grad_w2, grad_w1 = pl.pallas_call(
            functools.partial(lower_kernel, n_dev, n // LOW_TILE),
            grid=(CHUNKS, n // LOW_TILE),
            in_specs=[tile_spec(LOW_TILE), tile_spec(LOW_TILE), col_spec(LOW_TILE), back_spec],
            out_specs=[any_spec] * 2,
            out_shape=[jax.ShapeDtypeStruct((ff, d), F32), jax.ShapeDtypeStruct((d, ff), F32)],
            scratch_shapes=[pltpu.VMEM((LOW_TILE, side), BF16)] * 2 + scratch(side),
            compiler_params=params(2),
            name="lower",
        )(x, d_h2, a_one, w_two if TRANS_B else w_two.T)

        grad_w4 = jnp.concatenate([w4_a, w4_b], axis=0)
        grad_w3 = jnp.concatenate([w3_a, w3_b], axis=1)
        return grad_w1, grad_w2, grad_w3, grad_w4

    return jax.shard_map(
        device_step,
        mesh=mesh,
        in_specs=(batch_spec, batch_spec, whole_spec, whole_spec, whole_spec, whole_spec),
        out_specs=(whole_spec, whole_spec, whole_spec, whole_spec),
        check_vma=False,
    )
```
